32 devices in a mesh: row: 8 (over z, x), col: 4 (over y, core).
Axes of the slice: x: 2, y: 2, z: 4, core: 2. Of those that a mesh axis runs over, the one named last changes fastest.
Arguments:
- voltage: float32 [2, 4096, 16384], P(None, ('row', 'col')), may hold values from -6 to 6
- chirp_phase: float32 [16384, 4096], P(('row', 'col')), may hold values from -3.140625 to 3.140625
- filter_taps: float32 [8, 1024], replicated, may hold values from -0.0625 to 0.0625
Outputs:
- filterbank: float32 [2, 1024, 65536], P(None, None, ('row', 'col'))
The draws below stay inside these ranges and needn't reach their ends.
All inputs are finite; a program needn't handle non-finite values.
Results may differ from the reference program's by a relative error of at most 0.00015.
Values sent between devices are 32-bit elements; how exact they have to be, the bound alone decides.
No kernel may reach another device: no remote copies, remote signals or barrier semaphores. Data moves between devices by JAX's collectives and lax.ppermute only.
A program may use at most 192 MiB of HBM per device.

```python
import jax
import jax.numpy as jnp
from jax import lax

FFT_ROWS = 4096
FFT_COLS = 16384
CHANNELS = 1024
TAPS = 8
SPECTRA = 65536


def shard_levels(stream_key, shape, pieces, smallest, high):
    gain, own = 1.0, jax.random.fold_in(stream_key, 6)
    for axis_at, blocks in pieces:
        steps = jnp.exp(jax.random.uniform(jax.random.fold_in(own, axis_at), (blocks,), jnp.float32, smallest / len(pieces), high / len(pieces)))
        gain = gain * jnp.repeat(steps, shape[axis_at] // blocks).reshape([-1 if axis == axis_at else 1 for axis in range(len(shape))])
    return gain


def centred(key, extent, spread, bound, pieces=(), dtype=jnp.bfloat16):
    result = jax.random.normal(key, extent, jnp.float32) * spread
    if len(pieces) > 0:
        result = shard_levels(key, extent, pieces, -0.22, 0.18) * result
    return jnp.clip(result, min=-bound, max=bound).astype(dtype)


def setup_inputs(seed: int = 0) -> dict:
    key_list = jax.random.split(jax.random.key(seed), 4)
    return {
        "voltage": centred(key_list[0], (2, FFT_ROWS, FFT_COLS), 1.0, 6.0, ((1, 32),), jnp.float32),
        "chirp_phase": jnp.clip(jax.random.uniform(key_list[1], (FFT_COLS, FFT_ROWS), jnp.float32, -3.140625, 3.140625), -3.140625, 3.140625),
        "filter_taps": centred(key_list[2], (TAPS, CHANNELS), (TAPS * CHANNELS) ** -0.5, 0.0625, (), jnp.float32),
    }


def reference(voltage, chirp_phase, filter_taps):
    series = lax.complex(voltage[0], voltage[1]).reshape(-1)
    spectrum = jnp.fft.fft(series)
    rotation = lax.complex(jnp.cos(chirp_phase), jnp.sin(chirp_phase)).reshape(-1)
    cleaned = jnp.fft.ifft(spectrum * rotation)
    frames = cleaned.reshape(SPECTRA, CHANNELS)
    padded = jnp.pad(frames, ((TAPS - 1, 0), (0, 0)))
    weighted = jnp.zeros_like(frames)
    for tap_delay in range(TAPS):
        offset = TAPS - 1 - tap_delay
        weighted = weighted + filter_taps[tap_delay] * padded[offset:offset + SPECTRA]
    channels_out = jnp.fft.fft(weighted, axis=1)
    return jnp.stack([jnp.real(channels_out).T, jnp.imag(channels_out).T])
```

```python
import functools
import math

import jax
import jax.numpy as jnp
import numpy as np
from jax import lax
from jax.experimental import pallas as pl
from jax.experimental.pallas import tpu as pltpu
from jax.sharding import PartitionSpec as P

AXES = ("row", "col")
LANES = 128
SPAN = 64
VMEM_LIMIT = 58 * 1024 * 1024


def times_constant(value, angle_num, angle_den, sign):
    re, im = value
    num = angle_num % angle_den
    eighth = 8 * num
    if eighth % angle_den == 0:
        octant = (eighth // angle_den) * int(sign) % 8
        root = math.sqrt(0.5)
        if octant == 0:
            return re, im
        if octant == 1:
            return (re - im) * root, (re + im) * root
        if octant == 2:
            return -im, re
        if octant == 3:
            return (re + im) * -root, (re - im) * root
        if octant == 4:
            return -re, -im
        if octant == 5:
            return (im - re) * root, (re + im) * -root
        if octant == 6:
            return im, -re
        return (re + im) * root, (im - re) * root
    turn = sign * 2.0 * math.pi * num / angle_den
    c, s = math.cos(turn), math.sin(turn)
    return re * c - im * s, re * s + im * c


def add(a, b):
    return a[0] + b[0], a[1] + b[1]


def sub(a, b):
    return a[0] - b[0], a[1] - b[1]


def dft4(x, sign):
    s0, d0 = add(x[0], x[2]), sub(x[0], x[2])
    s1, d1 = add(x[1], x[3]), sub(x[1], x[3])
    if sign < 0:
        y1 = (d0[0] + d1[1], d0[1] - d1[0])
        y3 = (d0[0] - d1[1], d0[1] + d1[0])
    else:
        y1 = (d0[0] - d1[1], d0[1] + d1[0])
        y3 = (d0[0] + d1[1], d0[1] - d1[0])
    return [add(s0, s1), y1, sub(s0, s1), y3]


def dft(x, sign):
    n = len(x)
    if n == 1:
        return x
    if n == 2:
        return [add(x[0], x[1]), sub(x[0], x[1])]
    if n == 4:
        return dft4(x, sign)
    quarter = n // 4
    parts = [dft(x[r::4], sign) for r in range(4)]
    result = [None] * n
    for k in range(quarter):
        turned = [times_constant(parts[r][k], r * k, n, sign) for r in range(4)]
        for q, value in enumerate(dft4(turned, sign)):
            result[k + q * quarter] = value
    return result


def dft_two_pass(size, sign, load, store, scratch):
    inner = min(size, 8)
    outer = size // inner
    for b in range(inner):
        values = dft([load(inner * a + b) for a in range(outer)], sign)
        for ka in range(outer):
            re, im = times_constant(values[ka], b * ka, size, sign)
            scratch[b * outer + ka, 0] = re
            scratch[b * outer + ka, 1] = im
    for ka in range(outer):
        group = [(scratch[b * outer + ka, 0], scratch[b * outer + ka, 1]) for b in range(inner)]
        for kb, value in enumerate(dft(group, sign)):
            store(ka + outer * kb, value)


def split_table(table):
    high = table.astype(jnp.bfloat16)
    low = (table - high.astype(np.float32)).astype(jnp.bfloat16)
    return high, low


def dft_matrix(size, sign, scale=1.0):
    digits = np.arange(size)
    turn = sign * 2.0 * np.pi * (digits[:, None] * digits[None, :] % size) / size
    c, s = np.cos(turn) * scale, np.sin(turn) * scale
    return np.block([[c, -s], [s, c]]).astype(np.float32)


def left_table(size, sign, scale=1.0):
    high, low = split_table(dft_matrix(size, sign, scale))
    return np.concatenate([high, high, low], axis=1)


def right_table(size, sign, scale=1.0):
    high, low = split_table(dft_matrix(size, sign, scale).T)
    return np.concatenate([high, high, low], axis=0)


def lane_twist(leads, length):
    turn = -2.0 * np.pi * (np.arange(leads)[:, None] * np.arange(LANES)[None, :] % length) / length
    return np.stack([np.cos(turn), np.sin(turn)], axis=1).astype(np.float32)


def halves(value):
    high = value.astype(jnp.bfloat16)
    low = (value - high.astype(jnp.float32)).astype(jnp.bfloat16)
    return high, low


def turn_by(re, im, c, s):
    return re * c - im * s, re * s + im * c


def turn_back(re, im, c, s):
    return re * c + im * s, im * c - re * s


def call(kernel, **options):
    cost = pl.CostEstimate(flops=options.pop("flops"), bytes_accessed=options.pop("bytes"), transcendentals=0)
    params = pltpu.CompilerParams(vmem_limit_bytes=VMEM_LIMIT)
    return pl.pallas_call(kernel, compiler_params=params, cost_estimate=cost, **options)


def deal(voltage, devices):
    rows, cols = voltage.shape[1:]
    chunks = cols // devices // LANES
    group = 4

    def kernel(x_ref, o_ref):
        for d in range(group):
            for c in range(chunks):
                at = (d * chunks + c) * LANES
                o_ref[d, c] = x_ref[:, :, at : at + LANES]

    return call(
        kernel,
        grid=(devices // group,),
        in_specs=[pl.BlockSpec((2, rows, group * chunks * LANES), lambda g: (0, 0, g))],
        out_specs=pl.BlockSpec((group, chunks, 2, rows, LANES), lambda g: (g, 0, 0, 0, 0)),
        out_shape=jax.ShapeDtypeStruct((devices, chunks, 2, rows, LANES), jnp.float32),
        flops=voltage.size,
        bytes=voltage.size * 8,
    )(voltage)


def columns_forward(values, inner_twist, twist):
    devices, chunks, _, rows, _ = values.shape
    table = jnp.asarray(left_table(rows, -1.0))
    tile = min(rows, 16)

    def kernel(x_ref, w_ref, tw_ref, t_ref, o_ref, pass_ref, mat_ref):
        def gather(step, carry):
            at = pl.ds(pl.multiple_of(step * tile, tile), tile)

            def load(s):
                return x_ref[s, 0, 0, at, :], x_ref[s, 0, 1, at, :]

            def store(k, value):
                re, im = turn_by(*value, tw_ref[0, k, at, :], tw_ref[1, k, at, :])
                lanes = slice((k % 2) * LANES, (k % 2 + 1) * LANES)
                for part, v in enumerate((re, im)):
                    high, low = halves(v)
                    for block, piece in ((part, high), (2 + part, low), (4 + part, high)):
                        rows_at = pl.ds(pl.multiple_of(block * rows + step * tile, tile), tile)
                        mat_ref[k // 2, rows_at, lanes] = piece

            dft_two_pass(devices, -1.0, load, store, pass_ref)
            return carry

        lax.fori_loop(0, rows // tile, gather, 0)

        def multiply(q, carry):
            product = jnp.dot(w_ref[...], mat_ref[q], preferred_element_type=jnp.float32)
            for h in range(2):
                lanes = slice(h * LANES, (h + 1) * LANES)
                k = 2 * q + h
                re, im = turn_by(product[:rows, lanes], product[rows:, lanes], t_ref[0, 0, k], t_ref[0, 1, k])
                o_ref[k, 0, 0] = re
                o_ref[k, 0, 1] = im
            return carry

        lax.fori_loop(0, devices // 2, multiply, 0)

    block = pl.BlockSpec((devices, 1, 2, rows, LANES), lambda c: (0, c, 0, 0, 0))
    return call(
        kernel,
        grid=(chunks,),
        in_specs=[
            block,
            pl.BlockSpec(table.shape, lambda c: (0, 0)),
            pl.BlockSpec(inner_twist.shape, lambda c: (0, 0, 0, 0)),
            pl.BlockSpec((1, 2, devices, rows, LANES), lambda c: (c, 0, 0, 0, 0)),
        ],
        out_specs=block,
        out_shape=jax.ShapeDtypeStruct(values.shape, jnp.float32),
        scratch_shapes=[
            pltpu.VMEM((devices, 2, tile, LANES), jnp.float32),
            pltpu.VMEM((devices // 2, 6 * rows, 2 * LANES), jnp.bfloat16),
        ],
        flops=values.size * 6 * rows * 2,
        bytes=values.size * 12,
    )(values, table, inner_twist, twist)


def columns_inverse(parts, inner_twist, twist, scale, first, count):
    devices = parts[0].shape[0]
    cuts = [part.shape[3] for part in parts]
    rows = sum(cuts)
    table = jnp.asarray(left_table(rows, 1.0, scale))
    tile = 8

    def kernel(*refs):
        x_refs = refs[: len(parts)]
        w_ref, tw_ref, t_ref, o_ref, mat_ref, mid_ref, pass_ref = refs[len(parts) :]

        def multiply(q, carry):
            for h in range(2):
                k = 2 * q + h
                lanes = slice(h * LANES, (h + 1) * LANES)
                at = 0
                for x_ref, cut in zip(x_refs, cuts):
                    cos_part = t_ref[0, 0, k, at : at + cut, :]
                    sin_part = t_ref[0, 1, k, at : at + cut, :]
                    turned = turn_back(x_ref[k, 0, 0], x_ref[k, 0, 1], cos_part, sin_part)
                    for part, v in enumerate(turned):
                        high, low = halves(v)
                        for piece_at, piece in ((part, high), (2 + part, low), (4 + part, high)):
                            mat_ref[piece_at * rows + at : piece_at * rows + at + cut, lanes] = piece
                    at += cut
            product = jnp.dot(w_ref[...], mat_ref[...], preferred_element_type=jnp.float32)
            for h in range(2):
                k = 2 * q + h
                lanes = slice(h * LANES, (h + 1) * LANES)
                re, im = turn_back(product[:rows, lanes], product[rows:, lanes], tw_ref[0, k], tw_ref[1, k])
                mid_ref[k, 0] = re
                mid_ref[k, 1] = im
            return carry

        lax.fori_loop(0, devices // 2, multiply, 0)

        def scatter(step, carry):
            at = pl.ds(pl.multiple_of(step * tile, tile), tile)

            def load(s):
                return mid_ref[s, 0, at, :], mid_ref[s, 1, at, :]

            def store(k, value):
                o_ref[k, 0, 0, at, :] = value[0]
                o_ref[k, 0, 1, at, :] = value[1]

            dft_two_pass(devices, 1.0, load, store, pass_ref)
            return carry

        lax.fori_loop(0, rows // tile, scatter, 0)

    def block(cut, start):
        return pl.BlockSpec((devices, 1, 2, cut, LANES), lambda c: (0, c + start, 0, 0, 0))

    size = devices * count * 2 * rows * LANES
    return call(
        kernel,
        grid=(count,),
        in_specs=[block(cut, first) for cut in cuts]
        + [
            pl.BlockSpec(table.shape, lambda c: (0, 0)),
            pl.BlockSpec(inner_twist.shape, lambda c: (0, 0, 0, 0)),
            pl.BlockSpec((1, 2, devices, rows, LANES), lambda c: (c + first, 0, 0, 0, 0)),
        ],
        out_specs=block(rows, 0),
        out_shape=jax.ShapeDtypeStruct((devices, count, 2, rows, LANES), jnp.float32),
        scratch_shapes=[
            pltpu.VMEM((6 * rows, 2 * LANES), jnp.bfloat16),
            pltpu.VMEM((devices, 2, rows, LANES), jnp.float32),
            pltpu.VMEM((devices, 2, tile, LANES), jnp.float32),
        ],
        flops=size * 6 * rows * 2,
        bytes=size * 12,
    )(*parts, table, inner_twist, twist)


def rows_filtered(values, cos_part, sin_part, first, count):
    leads = values.shape[0]
    tile = 8
    span = SPAN
    forward = jnp.asarray(right_table(LANES, -1.0))
    backward = jnp.asarray(right_table(LANES, 1.0))
    twist = jnp.asarray(lane_twist(leads, leads * LANES))
    inner = min(leads, 8)
    outer = leads // inner
    block_rows = span * tile

    def kernel(x_ref, c_ref, s_ref, f_ref, b_ref, tw_ref, o_ref, first_ref, left_ref, left2_ref, mid_ref):
        for b in range(inner):
            group = [(x_ref[inner * a + b, 0], x_ref[inner * a + b, 1]) for a in range(outer)]
            for ka, value in enumerate(dft(group, -1.0)):
                re, im = times_constant(value, b * ka, leads, -1.0)
                first_ref[b, 0, ka * tile : (ka + 1) * tile, :] = re
                first_ref[b, 1, ka * tile : (ka + 1) * tile, :] = im
        for pair in range(outer // 2):
            at = slice(pair * 2 * tile, (pair + 1) * 2 * tile)
            group = [(first_ref[b, 0, at, :], first_ref[b, 1, at, :]) for b in range(inner)]
            for kb, (re, im) in enumerate(dft(group, -1.0)):
                ka = 2 * pair + outer * kb
                c = jnp.concatenate([jnp.broadcast_to(tw_ref[ka + e, 0:1, :], (tile, LANES)) for e in range(2)], axis=0)
                s = jnp.concatenate([jnp.broadcast_to(tw_ref[ka + e, 1:2, :], (tile, LANES)) for e in range(2)], axis=0)
                re, im = turn_by(re, im, c, s)
                for part, v in enumerate((re, im)):
                    high, low = halves(v)
                    for piece_at, piece in ((part, high), (2 + part, low), (4 + part, high)):
                        left_ref[ka * tile : (ka + 2) * tile, piece_at * LANES : (piece_at + 1) * LANES] = piece

        def middle(step, carry):
            at = pl.ds(pl.multiple_of(step * block_rows, block_rows), block_rows)
            lead_at = pl.ds(pl.multiple_of(step * span, span), span)
            z = jnp.dot(left_ref[at, :], f_ref[...], preferred_element_type=jnp.float32)
            c = c_ref[lead_at].reshape(block_rows, LANES)
            s = s_ref[lead_at].reshape(block_rows, LANES)
            for part, v in enumerate(turn_by(z[:, :LANES], z[:, LANES:], c, s)):
                high, low = halves(v)
                for piece_at, piece in ((part, high), (2 + part, low), (4 + part, high)):
                    left2_ref[:, piece_at * LANES : (piece_at + 1) * LANES] = piece
            y = jnp.dot(left2_ref[...], b_ref[...], preferred_element_type=jnp.float32)
            y = y.reshape(span, tile, 2 * LANES)
            c = tw_ref[lead_at, 0:1, :]
            s = tw_ref[lead_at, 1:2, :]
            re, im = turn_back(y[:, :, :LANES], y[:, :, LANES:], c, s)
            mid_ref[lead_at, 0] = re
            mid_ref[lead_at, 1] = im
            return carry

        lax.fori_loop(0, leads // span, middle, 0)

        def load(k):
            return mid_ref[k, 0], mid_ref[k, 1]

        def store(j, value):
            o_ref[j, 0] = value[0]
            o_ref[j, 1] = value[1]

        for b in range(inner):
            group = dft([load(inner * a + b) for a in range(outer)], 1.0)
            for ka in range(outer):
                re, im = times_constant(group[ka], b * ka, leads, 1.0)
                first_ref[b, 0, ka * tile : (ka + 1) * tile, :] = re
                first_ref[b, 1, ka * tile : (ka + 1) * tile, :] = im
        for ka in range(outer):
            at = slice(ka * tile, (ka + 1) * tile)
            group = [(first_ref[b, 0, at, :], first_ref[b, 1, at, :]) for b in range(inner)]
            for kb, value in enumerate(dft(group, 1.0)):
                store(ka + outer * kb, value)

    chirp = pl.BlockSpec((leads, tile, LANES), lambda g: (0, g + first, 0))
    return call(
        kernel,
        grid=(count,),
        in_specs=[
            pl.BlockSpec((leads, 2, tile, LANES), lambda g: (0, 0, g + first, 0)),
            chirp,
            chirp,
            pl.BlockSpec(forward.shape, lambda g: (0, 0)),
            pl.BlockSpec(backward.shape, lambda g: (0, 0)),
            pl.BlockSpec(twist.shape, lambda g: (0, 0, 0)),
        ],
        out_specs=pl.BlockSpec((leads, 2, tile, LANES), lambda g: (0, 0, g, 0)),
        out_shape=jax.ShapeDtypeStruct((leads, 2, count * tile, LANES), jnp.float32),
        scratch_shapes=[
            pltpu.VMEM((inner, 2, outer * tile, LANES), jnp.float32),
            pltpu.VMEM((leads * tile, 6 * LANES), jnp.bfloat16),
            pltpu.VMEM((block_rows, 6 * LANES), jnp.bfloat16),
            pltpu.VMEM((leads, 2, tile, LANES), jnp.float32),
        ],
        flops=leads * 2 * count * tile * LANES * 6 * LANES * 4,
        bytes=leads * 2 * count * tile * LANES * 12,
    )(values, cos_part, sin_part, forward, backward, twist)


def where_lead(lead, parts):
    chunks = sum(part.shape[1] for part in parts)
    owner, chunk = lead // chunks, lead % chunks
    for number, part in enumerate(parts):
        if chunk < part.shape[1]:
            return number, owner, chunk
        chunk -= part.shape[1]


def last_frames(parts, past, pieces):
    rows = parts[0].shape[3]
    leads = sum(part.shape[0] * part.shape[1] for part in parts)
    tile = 8

    def kernel(*refs):
        o_ref = refs[-1]
        for e in range(past):
            for pa in range(pieces):
                number, owner, chunk = where_lead(leads - (past - e) * pieces + pa, parts)
                o_ref[e, pa] = refs[number][owner, chunk, :, tile - 1, :]

    def spec(part):
        return pl.BlockSpec(part.shape[:3] + (tile, LANES), lambda g: (0, 0, 0, rows // tile - 1, 0))

    return call(
        kernel,
        grid=(1,),
        in_specs=[spec(part) for part in parts],
        out_specs=pl.BlockSpec((past, pieces, 2, LANES), lambda g: (0, 0, 0, 0)),
        out_shape=jax.ShapeDtypeStruct((past, pieces, 2, LANES), jnp.float32),
        flops=leads * tile * LANES,
        bytes=leads * 2 * tile * LANES * 4,
    )(*parts)


def channelised(parts, history, filter_taps):
    rows = parts[0].shape[3]
    tap_count, channels = filter_taps.shape
    pieces = channels // LANES
    frames = sum(part.shape[0] * part.shape[1] for part in parts) // pieces
    taps = filter_taps.reshape(tap_count, pieces, LANES)
    past = tap_count - 1
    tile = 16
    table = jnp.asarray(left_table(LANES, -1.0))
    twist = jnp.asarray(lane_twist(pieces, channels))
    out_rows = tile * frames

    def kernel(*refs):
        x_refs = refs[: len(parts)]
        h_ref, taps_ref, w_ref, tw_ref, o_ref, ext_ref, last_ref, frame_ref, mat_ref, spread_ref = refs[len(parts) :]

        def at_lead(f, pa, part):
            number, owner, chunk = where_lead(f * pieces + pa, parts)
            return x_refs[number][owner, chunk, part]

        @pl.when(pl.program_id(0) == 0)
        def _():
            last_ref[...] = h_ref[...]

        first_row = lax.broadcasted_iota(jnp.int32, (tile, LANES), 0) == 0
        for e in range(past):
            for pa in range(pieces):
                for part in range(2):
                    x = at_lead(frames - past + e, pa, part)
                    before = jnp.broadcast_to(last_ref[e, pa, part : part + 1, :], (tile, LANES))
                    ext_ref[e, pa, part] = jnp.where(first_row, before, pltpu.roll(x, 1, 0))
                    last_ref[e, pa, part : part + 1, :] = x[tile - 1 : tile, :]
        for f in range(frames):
            for pa in range(pieces):
                for part in range(2):
                    ext_ref[past + f, pa, part] = at_lead(f, pa, part)

        def filtered(f, carry):
            group = []
            for pa in range(pieces):
                total = [None, None]
                for t in range(tap_count):
                    tap = taps_ref[t, pa : pa + 1, :]
                    for part in range(2):
                        term = ext_ref[f + past - t, pa, part] * tap
                        total[part] = term if total[part] is None else total[part] + term
                group.append(tuple(total))
            for ca, (re, im) in enumerate(dft(group, -1.0)):
                re, im = turn_by(re, im, tw_ref[ca, 0:1, :], tw_ref[ca, 1:2, :])
                frame_ref[ca, 0, pl.ds(f, tile, stride=frames), :] = re
                frame_ref[ca, 1, pl.ds(f, tile, stride=frames), :] = im
            return carry

        lax.fori_loop(0, frames, filtered, 0)

        for ca in range(pieces):
            for part in range(2):
                high, low = halves(frame_ref[ca, part])
                for piece_at, piece in ((part, high), (2 + part, low), (4 + part, high)):
                    mat_ref[:, piece_at * LANES : (piece_at + 1) * LANES] = piece
            y = lax.dot_general(
                w_ref[...], mat_ref[...], (((1,), (1,)), ((), ())), preferred_element_type=jnp.float32
            )
            for part in range(2):
                for h in range(out_rows // LANES):
                    block = y[part * LANES : (part + 1) * LANES, h * LANES : (h + 1) * LANES]
                    spread_ref[h, part, pl.ds(ca, LANES, stride=pieces), :] = block
        for h in range(out_rows // LANES):
            o_ref[:, :, h * LANES : (h + 1) * LANES] = spread_ref[h]

    return call(
        kernel,
        grid=(rows // tile,),
        in_specs=[pl.BlockSpec(part.shape[:3] + (tile, LANES), lambda g: (0, 0, 0, g, 0)) for part in parts]
        + [
            pl.BlockSpec(history.shape, lambda g: (0, 0, 0, 0)),
            pl.BlockSpec(taps.shape, lambda g: (0, 0, 0)),
            pl.BlockSpec(table.shape, lambda g: (0, 0)),
            pl.BlockSpec(twist.shape, lambda g: (0, 0, 0)),
        ],
        out_specs=pl.BlockSpec((2, channels, out_rows), lambda g: (0, 0, g)),
        out_shape=jax.ShapeDtypeStruct((2, channels, rows * frames), jnp.float32),
        scratch_shapes=[
            pltpu.VMEM((frames + past, pieces, 2, tile, LANES), jnp.float32),
            pltpu.VMEM(history.shape, jnp.float32),
            pltpu.VMEM((pieces, 2, out_rows, LANES), jnp.float32),
            pltpu.VMEM((out_rows, 6 * LANES), jnp.bfloat16),
            pltpu.VMEM((out_rows // LANES, 2, channels, LANES), jnp.float32),
        ],
        flops=rows * frames * channels * 2 * 6 * LANES * 2,
        bytes=rows * frames * channels * 2 * 8,
    )(*parts, history, taps, table, twist)


def exchange(values):
    return lax.all_to_all(values, AXES, split_axis=0, concat_axis=0, tiled=True)


def cut(count):
    if count == 1:
        return [(0, 1)]
    head = max(1, count // 4)
    return [(0, head), (head, count - head)]


def cos_sin(product, length, sign):
    turn = sign * 2.0 * math.pi / length * product.astype(jnp.float32)
    return jnp.stack([jnp.cos(turn), jnp.sin(turn)])


def local(voltage, chirp_phase, filter_taps):
    devices = lax.axis_size("row") * lax.axis_size("col")
    device = lax.axis_index(AXES)
    rows = voltage.shape[1]
    total_rows = rows * devices
    total_cols = voltage.shape[2]
    local_cols = total_cols // devices
    chunks = local_cols // LANES
    total = total_rows * total_cols
    leads = total_cols // LANES
    channels = filter_taps.shape[1]
    past = filter_taps.shape[0] - 1

    sent = deal(voltage, devices)
    got = exchange(sent)

    ks = jnp.arange(devices, dtype=jnp.int32)[:, None, None]
    kl = jnp.arange(rows, dtype=jnp.int32)[None, :, None]
    lane = jnp.arange(LANES, dtype=jnp.int32)[None, None, :]
    chunk = jnp.arange(chunks, dtype=jnp.int32)[:, None, None, None]
    column = device * local_cols + chunk * LANES + lane[None]
    k1 = (ks + devices * kl)[None]
    twist = jnp.moveaxis(cos_sin(k1 * column % total, total, -1.0), 0, 1)
    inner = jnp.broadcast_to(ks * kl % total_rows, (devices, rows, LANES))
    inner_twist = cos_sin(inner, total_rows, -1.0)

    phase = jnp.transpose(chirp_phase.reshape(local_cols, rows, devices), (2, 0, 1))
    phase = exchange(phase)
    phase = phase.reshape(leads, LANES, rows)
    phase = jnp.transpose(phase, (1, 2, 0))
    cos_part, sin_part = jnp.cos(phase), jnp.sin(phase)

    spread = columns_forward(got, inner_twist, twist)
    got = exchange(spread)
    got = got.reshape(leads, 2, rows, LANES)
    parts = []
    for first, count in cut(rows // 8):
        part = rows_filtered(got, cos_part, sin_part, first, count)
        parts.append(exchange(part.reshape(devices, chunks, 2, count * 8, LANES)))
    spans = []
    for first, count in cut(chunks):
        spans.append(exchange(columns_inverse(parts, inner_twist, twist, 1.0 / total, first, count)))

    route = [(d - 1, d) for d in range(1, devices)]
    history = lax.ppermute(last_frames(spans, past, channels // LANES), AXES, route)
    return channelised(spans, history, filter_taps)


def solution(mesh):
    in_specs = (P(None, AXES, None), P(AXES, None), P())
    out_specs = P(None, None, AXES)
    return jax.shard_map(local, mesh=mesh, in_specs=in_specs, out_specs=out_specs, check_vma=False)
```

```python
import functools
import math

import jax
import jax.numpy as jnp
import numpy as np
from jax import lax
from jax.experimental import pallas as pl
from jax.experimental.pallas import tpu as pltpu
from jax.sharding import PartitionSpec as P

AXES = ("row", "col")
LANES = 128
SPAN = 64
VMEM_LIMIT = 58 * 1024 * 1024


def times_constant(value, angle_num, angle_den, sign):
    re, im = value
    num = angle_num % angle_den
    eighth = 8 * num
    if eighth % angle_den == 0:
        octant = (eighth // angle_den) * int(sign) % 8
        root = math.sqrt(0.5)
        if octant == 0:
            return re, im
        if octant == 1:
            return (re - im) * root, (re + im) * root
        if octant == 2:
            return -im, re
        if octant == 3:
            return (re + im) * -root, (re - im) * root
        if octant == 4:
            return -re, -im
        if octant == 5:
            return (im - re) * root, (re + im) * -root
        if octant == 6:
            return im, -re
        return (re + im) * root, (im - re) * root
    turn = sign * 2.0 * math.pi * num / angle_den
    c, s = math.cos(turn), math.sin(turn)
    return re * c - im * s, re * s + im * c


def add(a, b):
    return a[0] + b[0], a[1] + b[1]


def sub(a, b):
    return a[0] - b[0], a[1] - b[1]


def dft4(x, sign):
    s0, d0 = add(x[0], x[2]), sub(x[0], x[2])
    s1, d1 = add(x[1], x[3]), sub(x[1], x[3])
    if sign < 0:
        y1 = (d0[0] + d1[1], d0[1] - d1[0])
        y3 = (d0[0] - d1[1], d0[1] + d1[0])
    else:
        y1 = (d0[0] - d1[1], d0[1] + d1[0])
        y3 = (d0[0] + d1[1], d0[1] - d1[0])
    return [add(s0, s1), y1, sub(s0, s1), y3]


def dft(x, sign):
    n = len(x)
    if n == 1:
        return x
    if n == 2:
        return [add(x[0], x[1]), sub(x[0], x[1])]
    if n == 4:
        return dft4(x, sign)
    quarter = n // 4
    parts = [dft(x[r::4], sign) for r in range(4)]
    result = [None] * n
    for k in range(quarter):
        turned = [times_constant(parts[r][k], r * k, n, sign) for r in range(4)]
        for q, value in enumerate(dft4(turned, sign)):
            result[k + q * quarter] = value
    return result


def dft_two_pass(size, sign, load, store, scratch):
    inner = min(size, 8)
    outer = size // inner
    for b in range(inner):
        values = dft([load(inner * a + b) for a in range(outer)], sign)
        for ka in range(outer):
            re, im = times_constant(values[ka], b * ka, size, sign)
            scratch[b * outer + ka, 0] = re
            scratch[b * outer + ka, 1] = im
    for ka in range(outer):
        group = [(scratch[b * outer + ka, 0], scratch[b * outer + ka, 1]) for b in range(inner)]
        for kb, value in enumerate(dft(group, sign)):
            store(ka + outer * kb, value)


def split_table(table):
    high = table.astype(jnp.bfloat16)
    low = (table - high.astype(np.float32)).astype(jnp.bfloat16)
    return high, low


def dft_matrix(size, sign, scale=1.0):
    digits = np.arange(size)
    turn = sign * 2.0 * np.pi * (digits[:, None] * digits[None, :] % size) / size
    c, s = np.cos(turn) * scale, np.sin(turn) * scale
    return np.block([[c, -s], [s, c]]).astype(np.float32)


def left_table(size, sign, scale=1.0):
    high, low = split_table(dft_matrix(size, sign, scale))
    return np.concatenate([high, high, low], axis=1)


def right_table(size, sign, scale=1.0):
    high, low = split_table(dft_matrix(size, sign, scale).T)
    return np.concatenate([high, high, low], axis=0)


def lane_twist(leads, length):
    turn = -2.0 * np.pi * (np.arange(leads)[:, None] * np.arange(LANES)[None, :] % length) / length
    return np.stack([np.cos(turn), np.sin(turn)], axis=1).astype(np.float32)


def halves(value):
    high = value.astype(jnp.bfloat16)
    low = (value - high.astype(jnp.float32)).astype(jnp.bfloat16)
    return high, low


def turn_by(re, im, c, s):
    return re * c - im * s, re * s + im * c


def turn_back(re, im, c, s):
    return re * c + im * s, im * c - re * s


def call(kernel, **options):
    cost = pl.CostEstimate(flops=options.pop("flops"), bytes_accessed=options.pop("bytes"), transcendentals=0)
    params = pltpu.CompilerParams(vmem_limit_bytes=VMEM_LIMIT)
    return pl.pallas_call(kernel, compiler_params=params, cost_estimate=cost, **options)


def deal(voltage, devices):
    rows, cols = voltage.shape[1:]
    chunks = cols // devices // LANES
    group = 4

    def kernel(x_ref, o_ref):
        for d in range(group):
            for c in range(chunks):
                at = (d * chunks + c) * LANES
                o_ref[d, c] = x_ref[:, :, at : at + LANES]

    return call(
        kernel,
        grid=(devices // group,),
        in_specs=[pl.BlockSpec((2, rows, group * chunks * LANES), lambda g: (0, 0, g))],
        out_specs=pl.BlockSpec((group, chunks, 2, rows, LANES), lambda g: (g, 0, 0, 0, 0)),
        out_shape=jax.ShapeDtypeStruct((devices, chunks, 2, rows, LANES), jnp.float32),
        flops=voltage.size,
        bytes=voltage.size * 8,
    )(voltage)


def columns_forward(values, inner_twist, twist):
    devices, chunks, _, rows, _ = values.shape
    table = jnp.asarray(left_table(rows, -1.0))
    tile = min(rows, 16)

    def kernel(x_ref, w_ref, tw_ref, t_ref, o_ref, pass_ref, mat_ref):
        def gather(step, carry):
            at = pl.ds(pl.multiple_of(step * tile, tile), tile)

            def load(s):
                return x_ref[s, 0, 0, at, :], x_ref[s, 0, 1, at, :]

            def store(k, value):
                re, im = turn_by(*value, tw_ref[0, k, at, :], tw_ref[1, k, at, :])
                lanes = slice((k % 2) * LANES, (k % 2 + 1) * LANES)
                for part, v in enumerate((re, im)):
                    high, low = halves(v)
                    for block, piece in ((part, high), (2 + part, low), (4 + part, high)):
                        rows_at = pl.ds(pl.multiple_of(block * rows + step * tile, tile), tile)
                        mat_ref[k // 2, rows_at, lanes] = piece

            dft_two_pass(devices, -1.0, load, store, pass_ref)
            return carry

        lax.fori_loop(0, rows // tile, gather, 0)

        def multiply(q, carry):
            product = jnp.dot(w_ref[...], mat_ref[q], preferred_element_type=jnp.float32)
            for h in range(2):
                lanes = slice(h * LANES, (h + 1) * LANES)
                k = 2 * q + h
                re, im = turn_by(product[:rows, lanes], product[rows:, lanes], t_ref[0, 0, k], t_ref[0, 1, k])
                o_ref[k, 0, 0] = re
                o_ref[k, 0, 1] = im
            return carry

        lax.fori_loop(0, devices // 2, multiply, 0)

    block = pl.BlockSpec((devices, 1, 2, rows, LANES), lambda c: (0, c, 0, 0, 0))
    return call(
        kernel,
        grid=(chunks,),
        in_specs=[
            block,
            pl.BlockSpec(table.shape, lambda c: (0, 0)),
            pl.BlockSpec(inner_twist.shape, lambda c: (0, 0, 0, 0)),
            pl.BlockSpec((1, 2, devices, rows, LANES), lambda c: (c, 0, 0, 0, 0)),
        ],
        out_specs=block,
        out_shape=jax.ShapeDtypeStruct(values.shape, jnp.float32),
        scratch_shapes=[
            pltpu.VMEM((devices, 2, tile, LANES), jnp.float32),
            pltpu.VMEM((devices // 2, 6 * rows, 2 * LANES), jnp.bfloat16),
        ],
        flops=values.size * 6 * rows * 2,
        bytes=values.size * 12,
    )(values, table, inner_twist, twist)


def columns_inverse(parts, inner_twist, twist, scale, first, count):
    devices = parts[0].shape[0]
    cuts = [part.shape[3] for part in parts]
    rows = sum(cuts)
    steps = 4
    share = devices // steps
    table = jnp.asarray(left_table(rows, 1.0, scale))
    tile = 8

    def kernel(*refs):
        x_refs = refs[: len(parts)]
        w_ref, tw_ref, t_ref, o_ref, mat_ref, mid_ref, pass_ref = refs[len(parts) :]
        base = pl.program_id(1) * share

        def multiply(q, carry):
            for h in range(2):
                k = 2 * q + h
                lanes = slice(h * LANES, (h + 1) * LANES)
                at = 0
                for x_ref, cut in zip(x_refs, cuts):
                    cos_part = t_ref[0, 0, k, at : at + cut, :]
                    sin_part = t_ref[0, 1, k, at : at + cut, :]
                    turned = turn_back(x_ref[k, 0, 0], x_ref[k, 0, 1], cos_part, sin_part)
                    for part, v in enumerate(turned):
                        high, low = halves(v)
                        for piece_at, piece in ((part, high), (2 + part, low), (4 + part, high)):
                            mat_ref[piece_at * rows + at : piece_at * rows + at + cut, lanes] = piece
                    at += cut
            product = jnp.dot(w_ref[...], mat_ref[...], preferred_element_type=jnp.float32)
            for h in range(2):
                k = 2 * q + h
                lanes = slice(h * LANES, (h + 1) * LANES)
                re, im = turn_back(product[:rows, lanes], product[rows:, lanes], tw_ref[0, k], tw_ref[1, k])
                mid_ref[base + k, 0] = re
                mid_ref[base + k, 1] = im
            return carry

        lax.fori_loop(0, share // 2, multiply, 0)

        def scatter(step, carry):
            at = pl.ds(pl.multiple_of(step * tile, tile), tile)

            def load(s):
                return mid_ref[s, 0, at, :], mid_ref[s, 1, at, :]

            def store(k, value):
                o_ref[k, 0, 0, at, :] = value[0]
                o_ref[k, 0, 1, at, :] = value[1]

            dft_two_pass(devices, 1.0, load, store, pass_ref)
            return carry

        @pl.when(pl.program_id(1) == steps - 1)
        def _():
            lax.fori_loop(0, rows // tile, scatter, 0)

    def block(cut):
        return pl.BlockSpec((share, 1, 2, cut, LANES), lambda c, s: (s, c + first, 0, 0, 0))

    size = devices * count * 2 * rows * LANES
    return call(
        kernel,
        grid=(count, steps),
        in_specs=[block(cut) for cut in cuts]
        + [
            pl.BlockSpec(table.shape, lambda c, s: (0, 0)),
            pl.BlockSpec((2, share, rows, LANES), lambda c, s: (0, s, 0, 0)),
            pl.BlockSpec((1, 2, share, rows, LANES), lambda c, s: (c + first, 0, s, 0, 0)),
        ],
        out_specs=pl.BlockSpec((devices, 1, 2, rows, LANES), lambda c, s: (0, c, 0, 0, 0)),
        out_shape=jax.ShapeDtypeStruct((devices, count, 2, rows, LANES), jnp.float32),
        scratch_shapes=[
            pltpu.VMEM((6 * rows, 2 * LANES), jnp.bfloat16),
            pltpu.VMEM((devices, 2, rows, LANES), jnp.float32),
            pltpu.VMEM((devices, 2, tile, LANES), jnp.float32),
        ],
        flops=size * 6 * rows * 2,
        bytes=size * 12,
    )(*parts, table, inner_twist, twist)


def rows_filtered(values, cos_part, sin_part, first, count):
    leads = values.shape[0]
    tile = 8
    span = SPAN
    forward = jnp.asarray(right_table(LANES, -1.0))
    backward = jnp.asarray(right_table(LANES, 1.0))
    twist = jnp.asarray(lane_twist(leads, leads * LANES))
    inner = min(leads, 8)
    outer = leads // inner
    block_rows = span * tile

    def kernel(x_ref, c_ref, s_ref, f_ref, b_ref, tw_ref, o_ref, first_ref, left_ref, left2_ref, mid_ref):
        for b in range(inner):
            group = [(x_ref[inner * a + b, 0], x_ref[inner * a + b, 1]) for a in range(outer)]
            for ka, value in enumerate(dft(group, -1.0)):
                re, im = times_constant(value, b * ka, leads, -1.0)
                first_ref[b, 0, ka * tile : (ka + 1) * tile, :] = re
                first_ref[b, 1, ka * tile : (ka + 1) * tile, :] = im
        for pair in range(outer // 2):
            at = slice(pair * 2 * tile, (pair + 1) * 2 * tile)
            group = [(first_ref[b, 0, at, :], first_ref[b, 1, at, :]) for b in range(inner)]
            for kb, (re, im) in enumerate(dft(group, -1.0)):
                ka = 2 * pair + outer * kb
                c = jnp.concatenate([jnp.broadcast_to(tw_ref[ka + e, 0:1, :], (tile, LANES)) for e in range(2)], axis=0)
                s = jnp.concatenate([jnp.broadcast_to(tw_ref[ka + e, 1:2, :], (tile, LANES)) for e in range(2)], axis=0)
                re, im = turn_by(re, im, c, s)
                for part, v in enumerate((re, im)):
                    high, low = halves(v)
                    for piece_at, piece in ((part, high), (2 + part, low), (4 + part, high)):
                        left_ref[ka * tile : (ka + 2) * tile, piece_at * LANES : (piece_at + 1) * LANES] = piece

        def middle(step, carry):
            at = pl.ds(pl.multiple_of(step * block_rows, block_rows), block_rows)
            lead_at = pl.ds(pl.multiple_of(step * span, span), span)
            z = jnp.dot(left_ref[at, :], f_ref[...], preferred_element_type=jnp.float32)
            c = c_ref[lead_at].reshape(block_rows, LANES)
            s = s_ref[lead_at].reshape(block_rows, LANES)
            for part, v in enumerate(turn_by(z[:, :LANES], z[:, LANES:], c, s)):
                high, low = halves(v)
                for piece_at, piece in ((part, high), (2 + part, low), (4 + part, high)):
                    left2_ref[:, piece_at * LANES : (piece_at + 1) * LANES] = piece
            y = jnp.dot(left2_ref[...], b_ref[...], preferred_element_type=jnp.float32)
            y = y.reshape(span, tile, 2 * LANES)
            c = tw_ref[lead_at, 0:1, :]
            s = tw_ref[lead_at, 1:2, :]
            re, im = turn_back(y[:, :, :LANES], y[:, :, LANES:], c, s)
            mid_ref[lead_at, 0] = re
            mid_ref[lead_at, 1] = im
            return carry

        lax.fori_loop(0, leads // span, middle, 0)

        def load(k):
            return mid_ref[k, 0], mid_ref[k, 1]

        def store(j, value):
            o_ref[j, 0] = value[0]
            o_ref[j, 1] = value[1]

        for b in range(inner):
            group = dft([load(inner * a + b) for a in range(outer)], 1.0)
            for ka in range(outer):
                re, im = times_constant(group[ka], b * ka, leads, 1.0)
                first_ref[b, 0, ka * tile : (ka + 1) * tile, :] = re
                first_ref[b, 1, ka * tile : (ka + 1) * tile, :] = im
        for ka in range(outer):
            at = slice(ka * tile, (ka + 1) * tile)
            group = [(first_ref[b, 0, at, :], first_ref[b, 1, at, :]) for b in range(inner)]
            for kb, value in enumerate(dft(group, 1.0)):
                store(ka + outer * kb, value)

    chirp = pl.BlockSpec((leads, tile, LANES), lambda g: (0, g + first, 0))
    return call(
        kernel,
        grid=(count,),
        in_specs=[
            pl.BlockSpec((leads, 2, tile, LANES), lambda g: (0, 0, g + first, 0)),
            chirp,
            chirp,
            pl.BlockSpec(forward.shape, lambda g: (0, 0)),
            pl.BlockSpec(backward.shape, lambda g: (0, 0)),
            pl.BlockSpec(twist.shape, lambda g: (0, 0, 0)),
        ],
        out_specs=pl.BlockSpec((leads, 2, tile, LANES), lambda g: (0, 0, g, 0)),
        out_shape=jax.ShapeDtypeStruct((leads, 2, count * tile, LANES), jnp.float32),
        scratch_shapes=[
            pltpu.VMEM((inner, 2, outer * tile, LANES), jnp.float32),
            pltpu.VMEM((leads * tile, 6 * LANES), jnp.bfloat16),
            pltpu.VMEM((block_rows, 6 * LANES), jnp.bfloat16),
            pltpu.VMEM((leads, 2, tile, LANES), jnp.float32),
        ],
        flops=leads * 2 * count * tile * LANES * 6 * LANES * 4,
        bytes=leads * 2 * count * tile * LANES * 12,
    )(values, cos_part, sin_part, forward, backward, twist)


def where_lead(lead, parts):
    chunks = sum(part.shape[1] for part in parts)
    owner, chunk = lead // chunks, lead % chunks
    for number, part in enumerate(parts):
        if chunk < part.shape[1]:
            return number, owner, chunk
        chunk -= part.shape[1]


def last_frames(parts, past, pieces):
    rows = parts[0].shape[3]
    leads = sum(part.shape[0] * part.shape[1] for part in parts)
    tile = 8

    def kernel(*refs):
        o_ref = refs[-1]
        for e in range(past):
            for pa in range(pieces):
                number, owner, chunk = where_lead(leads - (past - e) * pieces + pa, parts)
                o_ref[e, pa] = refs[number][owner, chunk, :, tile - 1, :]

    def spec(part):
        return pl.BlockSpec(part.shape[:3] + (tile, LANES), lambda g: (0, 0, 0, rows // tile - 1, 0))

    return call(
        kernel,
        grid=(1,),
        in_specs=[spec(part) for part in parts],
        out_specs=pl.BlockSpec((past, pieces, 2, LANES), lambda g: (0, 0, 0, 0)),
        out_shape=jax.ShapeDtypeStruct((past, pieces, 2, LANES), jnp.float32),
        flops=leads * tile * LANES,
        bytes=leads * 2 * tile * LANES * 4,
    )(*parts)


def channelised(parts, history, filter_taps):
    rows = parts[0].shape[3]
    tap_count, channels = filter_taps.shape
    pieces = channels // LANES
    frames = sum(part.shape[0] * part.shape[1] for part in parts) // pieces
    taps = filter_taps.reshape(tap_count, pieces, LANES)
    past = tap_count - 1
    tile = 16
    table = jnp.asarray(left_table(LANES, -1.0))
    twist = jnp.asarray(lane_twist(pieces, channels))
    out_rows = tile * frames
    pitch = frames + 1
    unroll = 4

    def kernel(*refs):
        x_refs = refs[: len(parts)]
        h_ref, taps_ref, w_ref, tw_ref, o_ref, sum_ref, last_ref, frame_ref, mat_ref, spread_ref = refs[len(parts) :]

        def at_lead(f, pa, part):
            number, owner, chunk = where_lead(f * pieces + pa, parts)
            return x_refs[number][owner, chunk, part]

        @pl.when(pl.program_id(0) == 0)
        def _():
            last_ref[...] = h_ref[...]

        first_row = lax.broadcasted_iota(jnp.int32, (tile, LANES), 0) == 0
        for pa in range(pieces):
            tap = [jnp.broadcast_to(taps_ref[t, pa : pa + 1, :], (tile, LANES)) for t in range(tap_count)]
            for part in range(2):
                series = []
                for e in range(past):
                    x = at_lead(frames - past + e, pa, part)
                    before = jnp.broadcast_to(last_ref[e, pa, part : part + 1, :], (tile, LANES))
                    series.append(jnp.where(first_row, before, pltpu.roll(x, 1, 0)))
                for f in range(frames):
                    series.append(at_lead(f, pa, part))
                    total = series[f + past] * tap[0]
                    for t in range(1, tap_count):
                        total = total + series[f + past - t] * tap[t]
                    sum_ref[f, pa, part] = total
                for e in range(past):
                    x = at_lead(frames - past + e, pa, part)
                    last_ref[e, pa, part : part + 1, :] = x[tile - 1 : tile, :]

        def pieces_dft(step, carry):
            for u in range(unroll):
                f = step * unroll + u
                group = [(sum_ref[f, pa, 0], sum_ref[f, pa, 1]) for pa in range(pieces)]
                for ca, (re, im) in enumerate(dft(group, -1.0)):
                    re, im = turn_by(re, im, tw_ref[ca, 0:1, :], tw_ref[ca, 1:2, :])
                    frame_ref[ca, 0, pl.ds(f, tile, stride=pitch), :] = re
                    frame_ref[ca, 1, pl.ds(f, tile, stride=pitch), :] = im
            return carry

        lax.fori_loop(0, frames // unroll, pieces_dft, 0)

        for ca in range(pieces):
            slot = ca % 2
            for part in range(2):
                for row in range(tile):
                    high, low = halves(frame_ref[ca, part, row * pitch : row * pitch + frames, :])
                    at = slice(row * frames, (row + 1) * frames)
                    for piece_at, piece in ((part, high), (2 + part, low), (4 + part, high)):
                        mat_ref[slot, at, piece_at * LANES : (piece_at + 1) * LANES] = piece
            y = lax.dot_general(
                w_ref[...], mat_ref[slot], (((1,), (1,)), ((), ())), preferred_element_type=jnp.float32
            )
            for part in range(2):
                for h in range(out_rows // LANES):
                    block = y[part * LANES : (part + 1) * LANES, h * LANES : (h + 1) * LANES]
                    spread_ref[h, part, pl.ds(ca, LANES, stride=pieces), :] = block
        for h in range(out_rows // LANES):
            o_ref[:, :, h * LANES : (h + 1) * LANES] = spread_ref[h]

    return call(
        kernel,
        grid=(rows // tile,),
        in_specs=[pl.BlockSpec(part.shape[:3] + (tile, LANES), lambda g: (0, 0, 0, g, 0)) for part in parts]
        + [
            pl.BlockSpec(history.shape, lambda g: (0, 0, 0, 0)),
            pl.BlockSpec(taps.shape, lambda g: (0, 0, 0)),
            pl.BlockSpec(table.shape, lambda g: (0, 0)),
            pl.BlockSpec(twist.shape, lambda g: (0, 0, 0)),
        ],
        out_specs=pl.BlockSpec((2, channels, out_rows), lambda g: (0, 0, g)),
        out_shape=jax.ShapeDtypeStruct((2, channels, rows * frames), jnp.float32),
        scratch_shapes=[
            pltpu.VMEM((frames, pieces, 2, tile, LANES), jnp.float32),
            pltpu.VMEM(history.shape, jnp.float32),
            pltpu.VMEM((pieces, 2, tile * pitch, LANES), jnp.float32),
            pltpu.VMEM((2, out_rows, 6 * LANES), jnp.bfloat16),
            pltpu.VMEM((out_rows // LANES, 2, channels, LANES), jnp.float32),
        ],
        flops=rows * frames * channels * 2 * 6 * LANES * 2,
        bytes=rows * frames * channels * 2 * 8,
    )(*parts, history, taps, table, twist)


def exchange(values):
    return lax.all_to_all(values, AXES, split_axis=0, concat_axis=0, tiled=True)


def cut(count, share):
    if count == 1:
        return [(0, 1)]
    head = max(1, count // share)
    return [(0, head), (head, count - head)]


def cos_sin(product, length, sign):
    turn = sign * 2.0 * math.pi / length * product.astype(jnp.float32)
    return jnp.stack([jnp.cos(turn), jnp.sin(turn)])


def local(voltage, chirp_phase, filter_taps):
    devices = lax.axis_size("row") * lax.axis_size("col")
    device = lax.axis_index(AXES)
    rows = voltage.shape[1]
    total_rows = rows * devices
    total_cols = voltage.shape[2]
    local_cols = total_cols // devices
    chunks = local_cols // LANES
    total = total_rows * total_cols
    leads = total_cols // LANES
    channels = filter_taps.shape[1]
    past = filter_taps.shape[0] - 1

    sent = deal(voltage, devices)
    got = exchange(sent)

    ks = jnp.arange(devices, dtype=jnp.int32)[:, None, None]
    kl = jnp.arange(rows, dtype=jnp.int32)[None, :, None]
    lane = jnp.arange(LANES, dtype=jnp.int32)[None, None, :]
    chunk = jnp.arange(chunks, dtype=jnp.int32)[:, None, None, None]
    column = device * local_cols + chunk * LANES + lane[None]
    k1 = (ks + devices * kl)[None]
    twist = jnp.moveaxis(cos_sin(k1 * column % total, total, -1.0), 0, 1)
    inner = jnp.broadcast_to(ks * kl % total_rows, (devices, rows, LANES))
    inner_twist = cos_sin(inner, total_rows, -1.0)

    phase = jnp.transpose(chirp_phase.reshape(local_cols, rows, devices), (2, 0, 1))
    phase = exchange(phase)
    phase = phase.reshape(leads, LANES, rows)
    phase = jnp.transpose(phase, (1, 2, 0))
    cos_part, sin_part = jnp.cos(phase), jnp.sin(phase)

    spread = columns_forward(got, inner_twist, twist)
    got = exchange(spread)
    got = got.reshape(leads, 2, rows, LANES)
    parts = []
    for first, count in cut(rows // 8, 8):
        part = rows_filtered(got, cos_part, sin_part, first, count)
        parts.append(exchange(part.reshape(devices, chunks, 2, count * 8, LANES)))
    spans = []
    for first, count in cut(chunks, 4):
        spans.append(exchange(columns_inverse(parts, inner_twist, twist, 1.0 / total, first, count)))

    route = [(d - 1, d) for d in range(1, devices)]
    history = lax.ppermute(last_frames(spans, past, channels // LANES), AXES, route)
    return channelised(spans, history, filter_taps)


def solution(mesh):
    in_specs = (P(None, AXES, None), P(AXES, None), P())
    out_specs = P(None, None, AXES)
    return jax.shard_map(local, mesh=mesh, in_specs=in_specs, out_specs=out_specs, check_vma=False)
```

```python
import functools
import math

import jax
import jax.numpy as jnp
import numpy as np
from jax import lax
from jax.experimental import pallas as pl
from jax.experimental.pallas import tpu as pltpu
from jax.sharding import PartitionSpec as P

AXES = ("row", "col")
LANES = 128
SPAN = 64
VMEM_LIMIT = 58 * 1024 * 1024


def times_constant(value, angle_num, angle_den, sign):
    re, im = value
    num = angle_num % angle_den
    eighth = 8 * num
    if eighth % angle_den == 0:
        octant = (eighth // angle_den) * int(sign) % 8
        root = math.sqrt(0.5)
        if octant == 0:
            return re, im
        if octant == 1:
            return (re - im) * root, (re + im) * root
        if octant == 2:
            return -im, re
        if octant == 3:
            return (re + im) * -root, (re - im) * root
        if octant == 4:
            return -re, -im
        if octant == 5:
            return (im - re) * root, (re + im) * -root
        if octant == 6:
            return im, -re
        return (re + im) * root, (im - re) * root
    turn = sign * 2.0 * math.pi * num / angle_den
    c, s = math.cos(turn), math.sin(turn)
    return re * c - im * s, re * s + im * c


def add(a, b):
    return a[0] + b[0], a[1] + b[1]


def sub(a, b):
    return a[0] - b[0], a[1] - b[1]


def dft4(x, sign):
    s0, d0 = add(x[0], x[2]), sub(x[0], x[2])
    s1, d1 = add(x[1], x[3]), sub(x[1], x[3])
    if sign < 0:
        y1 = (d0[0] + d1[1], d0[1] - d1[0])
        y3 = (d0[0] - d1[1], d0[1] + d1[0])
    else:
        y1 = (d0[0] - d1[1], d0[1] + d1[0])
        y3 = (d0[0] + d1[1], d0[1] - d1[0])
    return [add(s0, s1), y1, sub(s0, s1), y3]


def dft(x, sign):
    n = len(x)
    if n == 1:
        return x
    if n == 2:
        return [add(x[0], x[1]), sub(x[0], x[1])]
    if n == 4:
        return dft4(x, sign)
    quarter = n // 4
    parts = [dft(x[r::4], sign) for r in range(4)]
    result = [None] * n
    for k in range(quarter):
        turned = [times_constant(parts[r][k], r * k, n, sign) for r in range(4)]
        for q, value in enumerate(dft4(turned, sign)):
            result[k + q * quarter] = value
    return result


def dft_two_pass(size, sign, load, store, scratch):
    inner = min(size, 8)
    outer = size // inner
    for b in range(inner):
        values = dft([load(inner * a + b) for a in range(outer)], sign)
        for ka in range(outer):
            re, im = times_constant(values[ka], b * ka, size, sign)
            scratch[b * outer + ka, 0] = re
            scratch[b * outer + ka, 1] = im
    for ka in range(outer):
        group = [(scratch[b * outer + ka, 0], scratch[b * outer + ka, 1]) for b in range(inner)]
        for kb, value in enumerate(dft(group, sign)):
            store(ka + outer * kb, value)


def split_table(table):
    high = table.astype(jnp.bfloat16)
    low = (table - high.astype(np.float32)).astype(jnp.bfloat16)
    return high, low


def dft_matrix(size, sign, scale=1.0):
    digits = np.arange(size)
    turn = sign * 2.0 * np.pi * (digits[:, None] * digits[None, :] % size) / size
    c, s = np.cos(turn) * scale, np.sin(turn) * scale
    return np.block([[c, -s], [s, c]]).astype(np.float32)


def left_table(size, sign, scale=1.0):
    high, low = split_table(dft_matrix(size, sign, scale))
    return np.concatenate([high, high, low], axis=1)


def right_table(size, sign, scale=1.0):
    high, low = split_table(dft_matrix(size, sign, scale).T)
    return np.concatenate([high, high, low], axis=0)


def lane_twist(leads, length):
    turn = -2.0 * np.pi * (np.arange(leads)[:, None] * np.arange(LANES)[None, :] % length) / length
    return np.stack([np.cos(turn), np.sin(turn)], axis=1).astype(np.float32)


def halves(value):
    high = value.astype(jnp.bfloat16)
    low = (value - high.astype(jnp.float32)).astype(jnp.bfloat16)
    return high, low


def turn_by(re, im, c, s):
    return re * c - im * s, re * s + im * c


def turn_back(re, im, c, s):
    return re * c + im * s, im * c - re * s


def call(kernel, **options):
    cost = pl.CostEstimate(flops=options.pop("flops"), bytes_accessed=options.pop("bytes"), transcendentals=0)
    params = pltpu.CompilerParams(vmem_limit_bytes=VMEM_LIMIT)
    return pl.pallas_call(kernel, compiler_params=params, cost_estimate=cost, **options)


def deal(voltage, devices):
    rows, cols = voltage.shape[1:]
    chunks = cols // devices // LANES
    group = 8

    def kernel(x_ref, o_ref):
        for d in range(group):
            for c in range(chunks):
                at = (d * chunks + c) * LANES
                o_ref[d, c] = x_ref[:, :, at : at + LANES]

    return call(
        kernel,
        grid=(devices // group,),
        in_specs=[pl.BlockSpec((2, rows, group * chunks * LANES), lambda g: (0, 0, g))],
        out_specs=pl.BlockSpec((group, chunks, 2, rows, LANES), lambda g: (g, 0, 0, 0, 0)),
        out_shape=jax.ShapeDtypeStruct((devices, chunks, 2, rows, LANES), jnp.float32),
        flops=voltage.size,
        bytes=voltage.size * 8,
    )(voltage)


def columns_forward(values, inner_twist, twist):
    devices, chunks, _, rows, _ = values.shape
    table = jnp.asarray(left_table(rows, -1.0))
    tile = min(rows, 16)

    def kernel(x_ref, w_ref, tw_ref, t_ref, o_ref, pass_ref, mat_ref):
        def gather(step, carry):
            at = pl.ds(pl.multiple_of(step * tile, tile), tile)

            def load(s):
                return x_ref[s, 0, 0, at, :], x_ref[s, 0, 1, at, :]

            def store(k, value):
                re, im = turn_by(*value, tw_ref[0, k, at, :], tw_ref[1, k, at, :])
                lanes = slice((k % 2) * LANES, (k % 2 + 1) * LANES)
                for part, v in enumerate((re, im)):
                    high, low = halves(v)
                    for block, piece in ((part, high), (2 + part, low), (4 + part, high)):
                        rows_at = pl.ds(pl.multiple_of(block * rows + step * tile, tile), tile)
                        mat_ref[k // 2, rows_at, lanes] = piece

            dft_two_pass(devices, -1.0, load, store, pass_ref)
            return carry

        lax.fori_loop(0, rows // tile, gather, 0)

        def multiply(q, carry):
            product = jnp.dot(w_ref[...], mat_ref[q], preferred_element_type=jnp.float32)
            for h in range(2):
                lanes = slice(h * LANES, (h + 1) * LANES)
                k = 2 * q + h
                re, im = turn_by(product[:rows, lanes], product[rows:, lanes], t_ref[0, 0, k], t_ref[0, 1, k])
                o_ref[k, 0, 0] = re
                o_ref[k, 0, 1] = im
            return carry

        lax.fori_loop(0, devices // 2, multiply, 0)

    block = pl.BlockSpec((devices, 1, 2, rows, LANES), lambda c: (0, c, 0, 0, 0))
    return call(
        kernel,
        grid=(chunks,),
        in_specs=[
            block,
            pl.BlockSpec(table.shape, lambda c: (0, 0)),
            pl.BlockSpec(inner_twist.shape, lambda c: (0, 0, 0, 0)),
            pl.BlockSpec((1, 2, devices, rows, LANES), lambda c: (c, 0, 0, 0, 0)),
        ],
        out_specs=block,
        out_shape=jax.ShapeDtypeStruct(values.shape, jnp.float32),
        scratch_shapes=[
            pltpu.VMEM((devices, 2, tile, LANES), jnp.float32),
            pltpu.VMEM((devices // 2, 6 * rows, 2 * LANES), jnp.bfloat16),
        ],
        flops=values.size * 6 * rows * 2,
        bytes=values.size * 12,
    )(values, table, inner_twist, twist)


def columns_inverse(parts, inner_twist, twist, scale, first, count):
    devices = parts[0].shape[0]
    cuts = [part.shape[3] for part in parts]
    rows = sum(cuts)
    steps = 4
    share = devices // steps
    table = jnp.asarray(left_table(rows, 1.0, scale))
    tile = 8

    def kernel(*refs):
        x_refs = refs[: len(parts)]
        w_ref, tw_ref, t_ref, o_ref, mat_ref, mid_ref, pass_ref = refs[len(parts) :]
        base = pl.program_id(1) * share

        def multiply(q, carry):
            for h in range(2):
                k = 2 * q + h
                lanes = slice(h * LANES, (h + 1) * LANES)
                at = 0
                for x_ref, cut in zip(x_refs, cuts):
                    cos_part = t_ref[0, 0, k, at : at + cut, :]
                    sin_part = t_ref[0, 1, k, at : at + cut, :]
                    turned = turn_back(x_ref[k, 0, 0], x_ref[k, 0, 1], cos_part, sin_part)
                    for part, v in enumerate(turned):
                        high, low = halves(v)
                        for piece_at, piece in ((part, high), (2 + part, low), (4 + part, high)):
                            mat_ref[piece_at * rows + at : piece_at * rows + at + cut, lanes] = piece
                    at += cut
            product = jnp.dot(w_ref[...], mat_ref[...], preferred_element_type=jnp.float32)
            for h in range(2):
                k = 2 * q + h
                lanes = slice(h * LANES, (h + 1) * LANES)
                re, im = turn_back(product[:rows, lanes], product[rows:, lanes], tw_ref[0, k], tw_ref[1, k])
                mid_ref[base + k, 0] = re
                mid_ref[base + k, 1] = im
            return carry

        lax.fori_loop(0, share // 2, multiply, 0)

        def scatter(step, carry):
            at = pl.ds(pl.multiple_of(step * tile, tile), tile)

            def load(s):
                return mid_ref[s, 0, at, :], mid_ref[s, 1, at, :]

            def store(k, value):
                o_ref[k, 0, 0, at, :] = value[0]
                o_ref[k, 0, 1, at, :] = value[1]

            dft_two_pass(devices, 1.0, load, store, pass_ref)
            return carry

        @pl.when(pl.program_id(1) == steps - 1)
        def _():
            lax.fori_loop(0, rows // tile, scatter, 0)

    def block(cut):
        return pl.BlockSpec((share, 1, 2, cut, LANES), lambda c, s: (s, c + first, 0, 0, 0))

    size = devices * count * 2 * rows * LANES
    return call(
        kernel,
        grid=(count, steps),
        in_specs=[block(cut) for cut in cuts]
        + [
            pl.BlockSpec(table.shape, lambda c, s: (0, 0)),
            pl.BlockSpec((2, share, rows, LANES), lambda c, s: (0, s, 0, 0)),
            pl.BlockSpec((1, 2, share, rows, LANES), lambda c, s: (c + first, 0, s, 0, 0)),
        ],
        out_specs=pl.BlockSpec((devices, 1, 2, rows, LANES), lambda c, s: (0, c, 0, 0, 0)),
        out_shape=jax.ShapeDtypeStruct((devices, count, 2, rows, LANES), jnp.float32),
        scratch_shapes=[
            pltpu.VMEM((6 * rows, 2 * LANES), jnp.bfloat16),
            pltpu.VMEM((devices, 2, rows, LANES), jnp.float32),
            pltpu.VMEM((devices, 2, tile, LANES), jnp.float32),
        ],
        flops=size * 6 * rows * 2,
        bytes=size * 12,
    )(*parts, table, inner_twist, twist)


def rows_filtered(values, cos_part, sin_part, first, count):
    leads = values.shape[0]
    tile = 8
    span = SPAN
    forward = jnp.asarray(right_table(LANES, -1.0))
    backward = jnp.asarray(right_table(LANES, 1.0))
    twist = jnp.asarray(lane_twist(leads, leads * LANES))
    inner = min(leads, 8)
    outer = leads // inner
    block_rows = span * tile

    def kernel(x_ref, c_ref, s_ref, f_ref, b_ref, tw_ref, o_ref, first_ref, left_ref, left2_ref, mid_ref):
        for b in range(inner):
            group = [(x_ref[inner * a + b, 0], x_ref[inner * a + b, 1]) for a in range(outer)]
            for ka, value in enumerate(dft(group, -1.0)):
                re, im = times_constant(value, b * ka, leads, -1.0)
                first_ref[b, 0, ka * tile : (ka + 1) * tile, :] = re
                first_ref[b, 1, ka * tile : (ka + 1) * tile, :] = im
        for pair in range(outer // 2):
            at = slice(pair * 2 * tile, (pair + 1) * 2 * tile)
            group = [(first_ref[b, 0, at, :], first_ref[b, 1, at, :]) for b in range(inner)]
            for kb, (re, im) in enumerate(dft(group, -1.0)):
                ka = 2 * pair + outer * kb
                c = jnp.concatenate([jnp.broadcast_to(tw_ref[ka + e, 0:1, :], (tile, LANES)) for e in range(2)], axis=0)
                s = jnp.concatenate([jnp.broadcast_to(tw_ref[ka + e, 1:2, :], (tile, LANES)) for e in range(2)], axis=0)
                re, im = turn_by(re, im, c, s)
                for part, v in enumerate((re, im)):
                    high, low = halves(v)
                    for piece_at, piece in ((part, high), (2 + part, low), (4 + part, high)):
                        left_ref[ka * tile : (ka + 2) * tile, piece_at * LANES : (piece_at + 1) * LANES] = piece

        def middle(step, carry):
            at = pl.ds(pl.multiple_of(step * block_rows, block_rows), block_rows)
            lead_at = pl.ds(pl.multiple_of(step * span, span), span)
            z = jnp.dot(left_ref[at, :], f_ref[...], preferred_element_type=jnp.float32)
            c = c_ref[lead_at].reshape(block_rows, LANES)
            s = s_ref[lead_at].reshape(block_rows, LANES)
            for part, v in enumerate(turn_by(z[:, :LANES], z[:, LANES:], c, s)):
                high, low = halves(v)
                for piece_at, piece in ((part, high), (2 + part, low), (4 + part, high)):
                    left2_ref[:, piece_at * LANES : (piece_at + 1) * LANES] = piece
            y = jnp.dot(left2_ref[...], b_ref[...], preferred_element_type=jnp.float32)
            y = y.reshape(span, tile, 2 * LANES)
            c = tw_ref[lead_at, 0:1, :]
            s = tw_ref[lead_at, 1:2, :]
            re, im = turn_back(y[:, :, :LANES], y[:, :, LANES:], c, s)
            mid_ref[lead_at, 0] = re
            mid_ref[lead_at, 1] = im
            return carry

        lax.fori_loop(0, leads // span, middle, 0)

        def load(k):
            return mid_ref[k, 0], mid_ref[k, 1]

        def store(j, value):
            o_ref[j, 0] = value[0]
            o_ref[j, 1] = value[1]

        for b in range(inner):
            group = dft([load(inner * a + b) for a in range(outer)], 1.0)
            for ka in range(outer):
                re, im = times_constant(group[ka], b * ka, leads, 1.0)
                first_ref[b, 0, ka * tile : (ka + 1) * tile, :] = re
                first_ref[b, 1, ka * tile : (ka + 1) * tile, :] = im
        for ka in range(outer):
            at = slice(ka * tile, (ka + 1) * tile)
            group = [(first_ref[b, 0, at, :], first_ref[b, 1, at, :]) for b in range(inner)]
            for kb, value in enumerate(dft(group, 1.0)):
                store(ka + outer * kb, value)

    chirp = pl.BlockSpec((leads, tile, LANES), lambda g: (0, g + first, 0))
    return call(
        kernel,
        grid=(count,),
        in_specs=[
            pl.BlockSpec((leads, 2, tile, LANES), lambda g: (0, 0, g + first, 0)),
            chirp,
            chirp,
            pl.BlockSpec(forward.shape, lambda g: (0, 0)),
            pl.BlockSpec(backward.shape, lambda g: (0, 0)),
            pl.BlockSpec(twist.shape, lambda g: (0, 0, 0)),
        ],
        out_specs=pl.BlockSpec((leads, 2, tile, LANES), lambda g: (0, 0, g, 0)),
        out_shape=jax.ShapeDtypeStruct((leads, 2, count * tile, LANES), jnp.float32),
        scratch_shapes=[
            pltpu.VMEM((inner, 2, outer * tile, LANES), jnp.float32),
            pltpu.VMEM((leads * tile, 6 * LANES), jnp.bfloat16),
            pltpu.VMEM((block_rows, 6 * LANES), jnp.bfloat16),
            pltpu.VMEM((leads, 2, tile, LANES), jnp.float32),
        ],
        flops=leads * 2 * count * tile * LANES * 6 * LANES * 4,
        bytes=leads * 2 * count * tile * LANES * 12,
    )(values, cos_part, sin_part, forward, backward, twist)


def where_lead(lead, parts):
    chunks = sum(part.shape[1] for part in parts)
    owner, chunk = lead // chunks, lead % chunks
    for number, part in enumerate(parts):
        if chunk < part.shape[1]:
            return number, owner, chunk
        chunk -= part.shape[1]


def last_frames(parts, past, pieces):
    rows = parts[0].shape[3]
    leads = sum(part.shape[0] * part.shape[1] for part in parts)
    tile = 8

    def kernel(*refs):
        o_ref = refs[-1]
        for e in range(past):
            for pa in range(pieces):
                number, owner, chunk = where_lead(leads - (past - e) * pieces + pa, parts)
                o_ref[e, pa] = refs[number][owner, chunk, :, tile - 1, :]

    def spec(part):
        return pl.BlockSpec(part.shape[:3] + (tile, LANES), lambda g: (0, 0, 0, rows // tile - 1, 0))

    return call(
        kernel,
        grid=(1,),
        in_specs=[spec(part) for part in parts],
        out_specs=pl.BlockSpec((past, pieces, 2, LANES), lambda g: (0, 0, 0, 0)),
        out_shape=jax.ShapeDtypeStruct((past, pieces, 2, LANES), jnp.float32),
        flops=leads * tile * LANES,
        bytes=leads * 2 * tile * LANES * 4,
    )(*parts)


def channelised(parts, history, filter_taps):
    rows = parts[0].shape[3]
    tap_count, channels = filter_taps.shape
    pieces = channels // LANES
    frames = sum(part.shape[0] * part.shape[1] for part in parts) // pieces
    past = tap_count - 1
    tile = 16
    table = jnp.asarray(right_table(LANES, -1.0))
    twist = jnp.asarray(lane_twist(pieces, channels))
    out_rows = tile * frames
    pitch = frames + 1
    together = 1

    def kernel(*refs):
        x_refs = refs[: len(parts)]
        h_ref, taps_ref, w_ref, tw_ref, o_ref, sum_ref, last_ref, frame_ref, mat_ref, spread_ref = refs[len(parts) :]

        def at_lead(f, pa, part):
            number, owner, chunk = where_lead(f * pieces + pa, parts)
            return x_refs[number][owner, chunk, part]

        @pl.when(pl.program_id(0) == 0)
        def _():
            last_ref[...] = h_ref[...]

        first_row = lax.broadcasted_iota(jnp.int32, (tile, LANES), 0) == 0

        def fir(pa):
            at = slice(pa * LANES, (pa + 1) * LANES)
            tap = [jnp.broadcast_to(taps_ref[t : t + 1, at], (tile, LANES)) for t in range(tap_count)]
            for part in range(2):
                series = []
                for e in range(past):
                    x = at_lead(frames - past + e, pa, part)
                    before = jnp.broadcast_to(last_ref[e, pa, part : part + 1, :], (tile, LANES))
                    series.append(jnp.where(first_row, before, pltpu.roll(x, 1, 0)))
                for f in range(frames):
                    series.append(at_lead(f, pa, part))
                    total = series[f + past] * tap[0]
                    for t in range(1, tap_count):
                        total = total + series[f + past - t] * tap[t]
                    sum_ref[f, pa, part] = total
                for e in range(past):
                    x = at_lead(frames - past + e, pa, part)
                    last_ref[e, pa, part : part + 1, :] = x[tile - 1 : tile, :]

        def pieces_dft(f):
            for first in range(0, tile, 8):
                at = slice(first, first + 8)
                group = [(sum_ref[f, pa, 0, at, :], sum_ref[f, pa, 1, at, :]) for pa in range(pieces)]
                for ca, (re, im) in enumerate(dft(group, -1.0)):
                    if ca > 0:
                        re, im = turn_by(re, im, tw_ref[ca, 0:1, :], tw_ref[ca, 1:2, :])
                    frame_ref[ca, 0, pl.ds(f + first * pitch, 8, stride=pitch), :] = re
                    frame_ref[ca, 1, pl.ds(f + first * pitch, 8, stride=pitch), :] = im

        def multiply(first):
            rows_at = slice(first * out_rows, (first + together) * out_rows)
            y = jnp.dot(mat_ref[rows_at, :], w_ref[...], preferred_element_type=jnp.float32)
            for ca in range(first, first + together):
                for part in range(2):
                    for h in range(out_rows // LANES):
                        at = (ca - first) * out_rows + h * LANES
                        block = y[at : at + LANES, part * LANES : (part + 1) * LANES]
                        spread_ref[h, part, pl.ds(ca, LANES, stride=pieces + 1), :] = jnp.transpose(block)

        for pa in range(pieces):
            fir(pa)
        for f in range(frames):
            pieces_dft(f)
        for ca in range(pieces):
            for part in range(2):
                for row in range(tile):
                    high, low = halves(frame_ref[ca, part, row * pitch : row * pitch + frames, :])
                    at = slice(ca * out_rows + row * frames, ca * out_rows + (row + 1) * frames)
                    for piece_at, piece in ((part, high), (2 + part, low), (4 + part, high)):
                        mat_ref[at, piece_at * LANES : (piece_at + 1) * LANES] = piece
            if (ca + 1) % together == 0:
                multiply(ca + 1 - together)
        for h in range(out_rows // LANES):
            for part in range(2):
                for cb in range(LANES):
                    tidy = spread_ref[h, part, cb * (pieces + 1) : cb * (pieces + 1) + pieces, :]
                    o_ref[part, cb * pieces : (cb + 1) * pieces, h * LANES : (h + 1) * LANES] = tidy

    tiles = rows // tile
    return call(
        kernel,
        grid=(tiles,),
        in_specs=[
            pl.BlockSpec(part.shape[:3] + (tile, LANES), lambda g: (0, 0, 0, g, 0))
            for part in parts
        ]
        + [
            pl.BlockSpec(history.shape, lambda g: (0, 0, 0, 0)),
            pl.BlockSpec(filter_taps.shape, lambda g: (0, 0)),
            pl.BlockSpec(table.shape, lambda g: (0, 0)),
            pl.BlockSpec(twist.shape, lambda g: (0, 0, 0)),
        ],
        out_specs=pl.BlockSpec((2, channels, out_rows), lambda g: (0, 0, g)),
        out_shape=jax.ShapeDtypeStruct((2, channels, rows * frames), jnp.float32),
        scratch_shapes=[
            pltpu.VMEM((frames, pieces, 2, tile, LANES), jnp.float32),
            pltpu.VMEM(history.shape, jnp.float32),
            pltpu.VMEM((pieces, 2, tile * pitch, LANES), jnp.float32),
            pltpu.VMEM((pieces * out_rows, 6 * LANES), jnp.bfloat16),
            pltpu.VMEM((out_rows // LANES, 2, channels + LANES, LANES), jnp.float32),
        ],
        flops=rows * frames * channels * 2 * 6 * LANES * 2,
        bytes=rows * frames * channels * 2 * 8,
    )(*parts, history, filter_taps, table, twist)


def exchange(values):
    return lax.all_to_all(values, AXES, split_axis=0, concat_axis=0, tiled=True)


def cut(count, share):
    if count == 1:
        return [(0, 1)]
    head = max(1, count // share)
    return [(0, head), (head, count - head)]


def cos_sin(product, length, sign):
    turn = sign * 2.0 * math.pi / length * product.astype(jnp.float32)
    return jnp.stack([jnp.cos(turn), jnp.sin(turn)])


def local(voltage, chirp_phase, filter_taps):
    devices = lax.axis_size("row") * lax.axis_size("col")
    device = lax.axis_index(AXES)
    rows = voltage.shape[1]
    total_rows = rows * devices
    total_cols = voltage.shape[2]
    local_cols = total_cols // devices
    chunks = local_cols // LANES
    total = total_rows * total_cols
    leads = total_cols // LANES
    channels = filter_taps.shape[1]
    past = filter_taps.shape[0] - 1

    sent = deal(voltage, devices)
    got = exchange(sent)

    ks = jnp.arange(devices, dtype=jnp.int32)[:, None, None]
    kl = jnp.arange(rows, dtype=jnp.int32)[None, :, None]
    lane = jnp.arange(LANES, dtype=jnp.int32)[None, None, :]
    chunk = jnp.arange(chunks, dtype=jnp.int32)[:, None, None, None]
    column = device * local_cols + chunk * LANES + lane[None]
    k1 = (ks + devices * kl)[None]
    twist = jnp.moveaxis(cos_sin(k1 * column % total, total, -1.0), 0, 1)
    inner = jnp.broadcast_to(ks * kl % total_rows, (devices, rows, LANES))
    inner_twist = cos_sin(inner, total_rows, -1.0)

    phase = jnp.transpose(chirp_phase.reshape(local_cols, rows, devices), (2, 0, 1))
    phase = exchange(phase)
    phase = phase.reshape(leads, LANES, rows)
    phase = jnp.transpose(phase, (1, 2, 0))
    cos_part, sin_part = jnp.cos(phase), jnp.sin(phase)

    spread = columns_forward(got, inner_twist, twist)
    got = exchange(spread)
    got = got.reshape(leads, 2, rows, LANES)
    parts = []
    for first, count in cut(rows // 8, 8):
        part = rows_filtered(got, cos_part, sin_part, first, count)
        parts.append(exchange(part.reshape(devices, chunks, 2, count * 8, LANES)))
    spans = []
    for first, count in cut(chunks, 4):
        spans.append(exchange(columns_inverse(parts, inner_twist, twist, 1.0 / total, first, count)))

    route = [(d - 1, d) for d in range(1, devices)]
    history = lax.ppermute(last_frames(spans, past, channels // LANES), AXES, route)
    return channelised(spans, history, filter_taps)


def solution(mesh):
    in_specs = (P(None, AXES, None), P(AXES, None), P())
    out_specs = P(None, None, AXES)
    return jax.shard_map(local, mesh=mesh, in_specs=in_specs, out_specs=out_specs, check_vma=False)
```
